32 devices in a mesh: seq: 8 (over y, x, core), tp: 4 (over z).
Axes of the slice: x: 2, y: 2, z: 4, core: 2. Of those that a mesh axis runs over, the one named last changes fastest.
Arguments:
- tokens: bfloat16 [4096, 3584], P('seq'), may hold values from -6 to 6
- norm_gain: float32 [3584], replicated, may hold values from 0.5 to 1.5
- q_weight: bfloat16 [3584, 3584], P(None, 'tp'), may hold values from -0.09375 to 0.09375
- q_bias: float32 [3584], P('tp'), may hold values from -9 to 9
- k_weight: bfloat16 [3584, 512], P(None, 'tp'), may hold values from -0.09375 to 0.09375
- k_bias: float32 [512], P('tp'), may hold values from -9 to 9
- v_weight: bfloat16 [3584, 512], P(None, 'tp'), may hold values from -0.09375 to 0.09375
- v_bias: float32 [512], P('tp'), may hold values from -5 to 5
- o_weight: bfloat16 [3584, 3584], P('tp'), may hold values from -0.09375 to 0.09375
- doc_ids: int32 [4096], replicated, may hold values from 0 to 7, never falling along the last dimension, each value on 1 to 2560 neighbouring positions
Outputs:
- attn_out: bfloat16 [4096, 3584], P('seq', 'tp')
The draws below stay inside these ranges and needn't reach their ends.
Inputs may be any that keep to these rules, and one draw needn't show every extreme that they name: `doc_ids`: document numbers never fall along the sequence; each document holds 1 to 2560 tokens and one holds exactly that many.
All inputs are finite; a program needn't handle non-finite values.
Results may differ from the reference program's by a relative error of at most 0.012.
Values may be sent and summed in bfloat16 or wider, within the bound.
A program may use at most 128 MiB of HBM per device.

```python
import math
import jax
import jax.numpy as jnp
import numpy as np
from jax import lax

D = 3584
HQ = 28
KVH = 4
HD = 128
TOK_DEV = 512
DOCS = 8
TOKENS = 4096
N_TP = 4


def bias_noise(key, count):
    return jnp.clip(jax.random.normal(key, (count,), jnp.float32), -5.0, 5.0)


def bias_plan(key):
    base = jax.random.fold_in(key, 9157)
    signs = (jax.random.randint(jax.random.fold_in(base, 1), (HD,), 0, 2) * 2 - 1).astype(jnp.float32)
    across = jnp.arange(HD) % (HD // 2)
    pattern = jnp.where(across >= HD // 2 - HD // 8, signs, 0.0)
    strong = jax.random.randint(jax.random.fold_in(base, 2), (), 0, KVH)
    order = jax.random.permutation(jax.random.fold_in(base, 3), HQ // KVH)
    levels = [115.0, -105.0, 60.0, 30.0]
    tops = jnp.concatenate([jnp.array(levels, jnp.float32), jnp.zeros((HQ // KVH - 4,), jnp.float32)])
    strength = tops[order]
    key_level = math.sqrt(4.0 * levels[0] / math.sqrt(HD))
    return (pattern, strong, strength, key_level)


def draw_k_bias(key, part):
    pattern, strong, strength, key_level = bias_plan(key)
    noise = bias_noise(jax.random.fold_in(key, 31), KVH * HD).reshape(KVH, HD)
    chosen = (jnp.arange(KVH) == strong)[:, None] & (pattern != 0.0)[None, :]
    return jnp.where(chosen, key_level * pattern[None, :], noise).reshape(KVH * HD).astype(jnp.float32)


def draw_q_bias(key, part):
    pattern, strong, strength, key_level = bias_plan(key)
    group = HQ // KVH
    noise = bias_noise(jax.random.fold_in(key, 37), HQ * HD).reshape(KVH, group, HD)
    level = 4.0 * strength / (math.sqrt(HD) * key_level)
    chosen = (jnp.arange(KVH) == strong)[:, None, None] & (strength != 0.0)[None, :, None] & (pattern != 0.0)[None, None, :]
    aligned = level[None, :, None] * pattern[None, None, :]
    return jnp.where(chosen, aligned, noise).reshape(HQ * HD).astype(jnp.float32)


def shard_levels(stream_key, extent, split, smallest, top_value):
    gain = 1.0
    for dim, shards_of in split:
        draws = jax.random.uniform(jax.random.fold_in(jax.random.fold_in(stream_key, 6), dim), (shards_of,), jnp.float32, smallest / len(split), top_value / len(split))
        gain = gain * jnp.repeat(jnp.exp(draws), extent[dim] // shards_of).reshape((-1,) + (1,) * (len(extent) - 1 - dim))
    return gain


def length_profile(amount, total, most, skew):
    portions = [(1 << 20) // math.isqrt(standing ** skew) + 1 for standing in range(2, amount + 1)]
    rest, given = total - most - (amount - 1), [1] * (amount - 1)
    while rest > 0:
        movable = [i for i in range(amount - 1) if given[i] < most]
        pool, left = sum([portions[i] for i in movable]), rest
        for i in movable:
            addition = min(most - given[i], max(1, left * portions[i] // pool), rest)
            given[i] = given[i] + addition
            rest = rest - addition
    return np.array([most] + given)


def uneven_parts(stream_key, amount, total, most, lean):
    if amount == 2:
        one = jax.random.randint(stream_key, (), max(1, total - most), min(most, total - 1) + 1)
        return jnp.stack([one, total - one])
    lengths = jnp.asarray(length_profile(amount, total, most, lean), jnp.int32)
    twos = (amount - 1) // 2
    giver, taker = lengths[1:1 + 2 * twos:2], lengths[2:2 + 2 * twos:2]
    slack = jnp.minimum(giver - 1, most - taker)
    moved = jax.random.randint(jax.random.fold_in(stream_key, 1), (twos,), 0, 1 << 20) % (slack + 1)
    lengths = lengths.at[1:1 + 2 * twos:2].set(giver - moved).at[2:2 + 2 * twos:2].set(taker + moved)
    return lengths[jax.random.permutation(jax.random.fold_in(stream_key, 2), amount)]


def normal_values(own_key, shape, scale, reach, split=(), held_as=jnp.bfloat16):
    values = jax.random.normal(own_key, shape, jnp.float32) * scale
    if len(split) > 0:
        values = shard_levels(own_key, shape, split, -0.22, 0.18) * values
    return jnp.clip(values, min=-reach, max=reach).astype(held_as)


def setup_inputs(seed: int = 0) -> dict:
    key_list = jax.random.split(jax.random.key(seed), 11)
    tokens = normal_values(key_list[0], (TOKENS, D), 1.0, 6.0, ((0, 8),))
    norm_gain = jnp.clip(1.0 + 0.1 * jax.random.normal(key_list[1], (D,), jnp.float32), 0.5, 1.5)
    q_weight = normal_values(key_list[2], (D, HQ * HD), D ** -0.5, 0.09375, ((1, 4),))
    q_bias = draw_q_bias(jax.random.fold_in(key_list[10], 71), 0)
    k_weight = normal_values(key_list[4], (D, KVH * HD), D ** -0.5, 0.09375, ((1, 4),))
    k_bias = draw_k_bias(jax.random.fold_in(key_list[10], 71), 0)
    v_weight = normal_values(key_list[6], (D, KVH * HD), D ** -0.5, 0.09375, ((1, 4),))
    v_bias = normal_values(key_list[7], (KVH * HD,), 1.0, 5.0, ((0, 4),), jnp.float32)
    o_weight = normal_values(key_list[8], (HQ * HD, D), (HQ * HD) ** -0.5, 0.09375, ((0, 4),))
    doc_ids = jnp.searchsorted(jnp.cumsum(uneven_parts(key_list[9], DOCS, TOKENS, TOKENS // 2 + TOK_DEV, 0)), jnp.arange(TOKENS), side="right").astype(jnp.int32)
    return {"tokens": tokens, "norm_gain": norm_gain, "q_weight": q_weight, "q_bias": q_bias, "k_weight": k_weight, "k_bias": k_bias, "v_weight": v_weight, "v_bias": v_bias, "o_weight": o_weight, "doc_ids": doc_ids}


rope_base = 1000000.0

def rotate(t, posf):
    half = t.shape[-1] // 2
    inv = rope_base ** (-(jnp.arange(half, dtype=jnp.float32) * 2.0) / t.shape[-1])
    angle = posf[:, None] * inv[None, :]
    angle = jnp.concatenate([angle, angle], axis=-1)
    turned = jnp.concatenate([-t[..., half:], t[..., :half]], axis=-1)
    return t * jnp.cos(angle)[:, None, :] + turned * jnp.sin(angle)[:, None, :]

def reference(tokens, norm_gain, q_weight, q_bias, k_weight, k_bias, v_weight, v_bias, o_weight, doc_ids):
    widened = tokens.astype(jnp.float32)
    normed = (widened * lax.rsqrt(lax.optimization_barrier(jnp.mean(widened * widened, axis=-1, keepdims=True)) + 1e-06) * norm_gain).astype(jnp.bfloat16)
    posf = jnp.arange(TOKENS).astype(jnp.float32)
    group = HQ // KVH
    query = jnp.dot(normed, q_weight, preferred_element_type=jnp.float32) + q_bias
    query = rotate(query.reshape(TOKENS, HQ, HD), posf).astype(jnp.bfloat16).reshape(TOKENS, KVH, group, HD)
    keys = jnp.dot(normed, k_weight, preferred_element_type=jnp.float32) + k_bias
    keys = rotate(keys.reshape(TOKENS, KVH, HD), posf).astype(jnp.bfloat16)
    values = (jnp.dot(normed, v_weight, preferred_element_type=jnp.float32) + v_bias).astype(jnp.bfloat16).reshape(TOKENS, KVH, HD)
    block = min(512, TOKENS)
    scale = 1.0 / HD ** 0.5
    kpos = jnp.arange(TOKENS).astype(jnp.int32)
    keys_f = keys.astype(jnp.float32)
    values_f = values.astype(jnp.float32)

    def attend(index):
        first = (index * block).astype(jnp.int32)
        qblock = lax.dynamic_slice_in_dim(query, first, block, 0).astype(jnp.float32)
        qdoc = lax.dynamic_slice_in_dim(doc_ids, first, block, 0)
        qpos = first + jnp.arange(block).astype(jnp.int32)
        scores = jnp.einsum('qkgd,tkd->kgqt', qblock, keys_f) * scale
        visible = (kpos[None, :] <= qpos[:, None]) & (qdoc[:, None] == doc_ids[None, :])
        scores = jnp.where(visible, scores, -1e+30)
        top = lax.optimization_barrier(jnp.max(scores, axis=-1, keepdims=True))
        expd = jnp.where(visible, jnp.exp(scores - top), 0.0)
        total = lax.optimization_barrier(jnp.sum(expd, axis=-1))
        weights = expd.astype(jnp.bfloat16).astype(jnp.float32)
        summed = jnp.einsum('kgqt,tkd->kgqd', weights, values_f) / total[..., None]
        return jnp.transpose(summed, (2, 0, 1, 3)).astype(jnp.bfloat16).reshape(block, HQ * HD)
    context = lax.map(attend, jnp.arange(TOKENS // block)).reshape(TOKENS, HQ * HD)
    width = HQ * HD // N_TP
    result = jnp.zeros((TOKENS, D), jnp.float32)
    for index in range(N_TP):
        term = jnp.dot(context[:, index * width:(index + 1) * width], o_weight[index * width:(index + 1) * width], preferred_element_type=jnp.float32)
        result = result + term.astype(jnp.bfloat16).astype(jnp.float32)
    return result.astype(jnp.bfloat16)
```

```python
import functools
import math

import jax
import jax.numpy as jnp
from jax import lax
from jax.experimental import pallas as pl
from jax.experimental.pallas import tpu as pltpu
from jax.sharding import PartitionSpec as P

HD = 128
MESH = pl.DeviceIdType.MESH
rope_base = 1000000.0
VMEM = pltpu.VMEM
LAG = 1


def rope_tables(first_row, rows):
    half = HD // 2
    inv = rope_base ** (-(jnp.arange(half, dtype=jnp.float32) * 2.0) / HD)
    posf = (first_row + jnp.arange(rows)).astype(jnp.float32)
    angle = posf[:, None] * inv[None, :]
    cos, sin = jnp.cos(angle), jnp.sin(angle)
    return jnp.concatenate([cos, cos], axis=-1), jnp.concatenate([-sin, sin], axis=-1)


def project(
    tokens_hbm, gain_ref, wq_hbm, qb_ref, wk_hbm, kb_ref, wv_hbm, vb_ref, cos_ref, sin_ref,
    q_ref, kv_ref, tokens, normed, wq, wkv, sems,
):
    width = wq.shape[1]
    step = 2 * HD
    spans = [(lo, min(step, width - lo)) for lo in range(0, width, step)]
    copies = [
        pltpu.make_async_copy(tokens_hbm, tokens, sems.at[0]),
        pltpu.make_async_copy(wk_hbm, wkv.at[:, pl.ds(0, HD)], sems.at[1]),
        pltpu.make_async_copy(wv_hbm, wkv.at[:, pl.ds(HD, HD)], sems.at[2]),
    ]
    for index, (lo, size) in enumerate(spans):
        cut = pl.ds(lo, size)
        copies.append(pltpu.make_async_copy(wq_hbm.at[:, cut], wq.at[:, cut], sems.at[3 + index]))
    for copy in copies:
        copy.start()
    copies[0].wait()
    rows = tokens.shape[0]
    piece = 64

    @pl.loop(0, rows // piece)
    def _(index):
        cut = pl.ds(pl.multiple_of(index * piece, piece), piece)
        wide = tokens[cut, :].astype(jnp.float32)
        mean = jnp.mean(wide * wide, axis=-1, keepdims=True)
        normed[cut, :] = (wide * lax.rsqrt(mean + 1e-06) * gain_ref[...]).astype(jnp.bfloat16)

    cos, sin = cos_ref[...], sin_ref[...]

    def rope(t):
        return (t * cos + pltpu.roll(t, HD // 2, 1) * sin).astype(jnp.bfloat16)

    copies[1].wait()
    copies[2].wait()
    kv = jnp.dot(normed[...], wkv[...], preferred_element_type=jnp.float32)
    kv_ref[0] = rope(kv[:, :HD] + kb_ref[...])
    kv_ref[1] = (kv[:, HD:] + vb_ref[...]).astype(jnp.bfloat16)
    for index, (lo, size) in enumerate(spans):
        copies[3 + index].wait()
        out = jnp.dot(
            normed[...], wq[:, lo:lo + size], preferred_element_type=jnp.float32
        ) + qb_ref[:, lo:lo + size]
        for head in range(0, size, HD):
            q_ref[:, lo + head:lo + head + HD] = rope(out[:, head:head + HD])


def attend(
    seq_count, tp_count, reach, chunk,
    q_ref, kv_ref, kdoc_ref, qdoc_ref, wo_hbm, out_ref,
    wo, kv_in, sent, got, own, wo_sem, kv_send, kv_recv, send_sem, recv_sem,
):
    place = lax.axis_index("seq")
    turn = lax.axis_index("tp")
    rows, width = q_ref.shape
    heads = width // HD
    cols = out_ref.shape[1]
    parts = rows // chunk
    load = pltpu.make_async_copy(wo_hbm, wo, wo_sem)
    load.start()

    barrier = pltpu.get_barrier_semaphore()
    for away in range(1, reach + 1):
        @pl.when(place >= away)
        def _():
            pl.semaphore_signal(barrier, inc=1, device_id={"seq": place - away}, device_id_type=MESH)

        @pl.when(place + away < seq_count)
        def _():
            pl.semaphore_signal(barrier, inc=1, device_id={"seq": place + away}, device_id_type=MESH)

    @pl.when(turn > 0)
    def _():
        pl.semaphore_signal(barrier, inc=1, device_id={"tp": turn - 1}, device_id_type=MESH)

    @pl.when(turn < tp_count - 1)
    def _():
        pl.semaphore_signal(barrier, inc=1, device_id={"tp": turn + 1}, device_id_type=MESH)

    behind = jnp.minimum(place, reach)
    ahead = jnp.minimum(seq_count - 1 - place, reach)
    sides = jnp.where(turn > 0, 1, 0) + jnp.where(turn < tp_count - 1, 1, 0)
    pl.semaphore_wait(barrier, behind + ahead + sides)

    def kv_copy(away):
        return pltpu.make_async_remote_copy(
            src_ref=kv_ref, dst_ref=kv_in.at[away - 1],
            send_sem=kv_send.at[away - 1], recv_sem=kv_recv.at[away - 1],
            device_id={"seq": lax.rem(place + away, seq_count)}, device_id_type=MESH,
        )

    for away in range(1, reach + 1):
        @pl.when(place + away < seq_count)
        def _():
            kv_copy(away).start()

    def term_copy(side, dest, part):
        cut = pl.ds(pl.multiple_of(part * chunk, chunk), chunk)
        target = lax.rem(turn + (1 if side == 0 else tp_count - 1), tp_count)
        return pltpu.make_async_remote_copy(
            src_ref=sent.at[dest, cut], dst_ref=got.at[side, dest, cut],
            send_sem=send_sem.at[dest, part], recv_sem=recv_sem.at[side, dest, part],
            device_id={"tp": target}, device_id_type=MESH,
        )

    factor = math.log2(math.e) / HD**0.5
    order = sorted(range(tp_count), key=lambda d: (-abs(2 * d - tp_count + 1), -d))

    def forward(part):
        cut = pl.ds(pl.multiple_of(part * chunk, chunk), chunk)
        for dest in order:
            for side in (0, 1):
                inner = (turn > 0) & (dest > turn) if side == 0 else (
                    (turn < tp_count - 1) & (dest < turn))

                @pl.when(inner)
                def _():
                    term_copy(side, dest, part).wait_recv()
                    sent[dest, cut] = (
                        sent[dest, cut].astype(jnp.float32) + got[side, dest, cut].astype(jnp.float32)
                    ).astype(jnp.bfloat16)
                    term_copy(side, dest, part).start()

    def finish(part):
        cut = pl.ds(pl.multiple_of(part * chunk, chunk), chunk)
        for dest in range(tp_count):
            for side in (0, 1):
                edge = (turn > 0) if side == 0 else (turn < tp_count - 1)

                @pl.when((dest == turn) & edge)
                def _():
                    term_copy(side, dest, part).wait_recv()
                    own[cut, :] = own[cut, :] + got[side, dest, cut].astype(jnp.float32)

        out_ref[cut, :] = own[cut, :].astype(jnp.bfloat16)

    def piece(part):
        cut = pl.ds(pl.multiple_of(part * chunk, chunk), chunk)
        q = jnp.concatenate([q_ref[cut, h * HD:(h + 1) * HD] for h in range(heads)], axis=0)
        qdoc = qdoc_ref[cut, :]

        def block(state, k, v, visible):
            top, total, summed = state
            s = lax.dot_general(q, k, (((1,), (1,)), ((), ())), preferred_element_type=jnp.float32)
            s = s.reshape(heads, chunk, rows) * factor
            s = jnp.where(visible[None], s, -1e30)
            fresh = jnp.maximum(top, jnp.max(s, axis=-1, keepdims=True))
            e = jnp.exp2(s - fresh)
            scale = jnp.exp2(top - fresh)
            total = total * scale + jnp.sum(e, axis=-1, keepdims=True)
            pv = jnp.dot(
                e.astype(jnp.bfloat16).reshape(heads * chunk, rows), v,
                preferred_element_type=jnp.float32,
            )
            return fresh, total, summed * scale + pv.reshape(heads, chunk, HD)

        row = part * chunk + lax.broadcasted_iota(jnp.int32, (chunk, rows), 0)
        col = lax.broadcasted_iota(jnp.int32, (chunk, rows), 1)
        state = (
            jnp.full((heads, chunk, 1), -1e30, jnp.float32),
            jnp.zeros((heads, chunk, 1), jnp.float32),
            jnp.zeros((heads, chunk, HD), jnp.float32),
        )
        state = block(
            state, kv_ref[0], kv_ref[1], (col <= row) & (qdoc == kdoc_ref[place])
        )

        def earlier(away, state):
            @pl.when(part == 0)
            def _():
                kv_copy(away).wait_recv()

            return block(
                state, kv_in[away - 1, 0], kv_in[away - 1, 1], qdoc == kdoc_ref[place - away]
            )

        _, total, summed = lax.fori_loop(1, behind + 1, earlier, state)
        context = (summed / total).astype(jnp.bfloat16)
        context = jnp.concatenate([context[h] for h in range(heads)], axis=1)

        @pl.when(part == 0)
        def _():
            load.wait()

        for dest in order:
            term = jnp.dot(
                context, wo[:, dest * cols:(dest + 1) * cols], preferred_element_type=jnp.float32
            )

            @pl.when(dest == turn)
            def _():
                own[cut, :] = term

            @pl.when(dest != turn)
            def _():
                sent[dest, cut] = term.astype(jnp.bfloat16)

            @pl.when((turn == 0) & (dest > 0))
            def _():
                term_copy(0, dest, part).start()

            @pl.when((turn == tp_count - 1) & (dest < tp_count - 1))
            def _():
                term_copy(1, dest, part).start()

    @pl.loop(0, parts + LAG)
    def _(part):
        @pl.when(part < parts)
        def _():
            piece(part)

        @pl.when(part >= LAG)
        def _():
            forward(part - LAG)

    @pl.loop(0, parts)
    def _(part):
        finish(part)

    @pl.loop(0, parts)
    def _(part):
        for dest in range(tp_count):
            @pl.when(dest != turn)
            def _():
                term_copy(0, dest, part).wait_send()

    for away in range(1, reach + 1):
        @pl.when(place + away < seq_count)
        def _():
            kv_copy(away).wait_send()


def body(
    tokens, norm_gain, q_weight, q_bias, k_weight, k_bias, v_weight, v_bias, o_weight, doc_ids
):
    rows, model = tokens.shape
    seq_count = lax.axis_size("seq")
    tp_count = lax.axis_size("tp")
    place = lax.axis_index("seq")
    width = q_weight.shape[1]
    cols = o_weight.shape[1] // tp_count
    reach = min(seq_count - 1, (seq_count * rows // 2 + 2 * rows - 2) // rows)
    chunk = rows // 4
    parts = rows // chunk
    cos, sin = rope_tables(place * rows, rows)
    hbm = pl.BlockSpec(memory_space=pl.ANY)
    vmem = pl.BlockSpec(memory_space=VMEM)
    limit = 56 * 1024 * 1024
    query, kv = pl.pallas_call(
        project,
        out_shape=(
            jax.ShapeDtypeStruct((rows, width), jnp.bfloat16),
            jax.ShapeDtypeStruct((2, rows, HD), jnp.bfloat16),
        ),
        in_specs=[hbm, vmem, hbm, vmem, hbm, vmem, hbm, vmem, vmem, vmem],
        out_specs=(vmem, vmem),
        scratch_shapes=[
            VMEM((rows, model), jnp.bfloat16),
            VMEM((rows, model), jnp.bfloat16),
            VMEM((model, width), jnp.bfloat16),
            VMEM((model, 2 * HD), jnp.bfloat16),
            pltpu.SemaphoreType.DMA((3 + -(-width // (2 * HD)),)),
        ],
        compiler_params=pltpu.CompilerParams(vmem_limit_bytes=limit),
    )(
        tokens, norm_gain[None], q_weight, q_bias[None], k_weight, k_bias[None],
        v_weight, v_bias[None], cos, sin,
    )
    qdoc = lax.dynamic_slice_in_dim(doc_ids, place * rows, rows, 0)[:, None]
    kdoc = doc_ids.reshape(seq_count, 1, rows)
    return pl.pallas_call(
        functools.partial(attend, seq_count, tp_count, reach, chunk),
        out_shape=jax.ShapeDtypeStruct((rows, cols), jnp.bfloat16),
        in_specs=[vmem, vmem, vmem, vmem, hbm],
        out_specs=vmem,
        scratch_shapes=[
            VMEM(o_weight.shape, jnp.bfloat16),
            VMEM((reach, 2, rows, HD), jnp.bfloat16),
            VMEM((tp_count, rows, cols), jnp.bfloat16),
            VMEM((2, tp_count, rows, cols), jnp.bfloat16),
            VMEM((rows, cols), jnp.float32),
            pltpu.SemaphoreType.DMA,
            pltpu.SemaphoreType.DMA((reach,)),
            pltpu.SemaphoreType.DMA((reach,)),
            pltpu.SemaphoreType.DMA((tp_count, parts)),
            pltpu.SemaphoreType.DMA((2, tp_count, parts)),
        ],
        compiler_params=pltpu.CompilerParams(
            collective_id=0, has_side_effects=True, vmem_limit_bytes=limit
        ),
    )(query, kv, kdoc, qdoc, o_weight)


def solution(mesh):
    placed = (
        P("seq", None),
        P(),
        P(None, "tp"),
        P("tp"),
        P(None, "tp"),
        P("tp"),
        P(None, "tp"),
        P("tp"),
        P("tp", None),
        P(),
    )
    return jax.shard_map(
        body, mesh=mesh, in_specs=placed, out_specs=P("seq", "tp"), check_vma=False
    )
```

```python
import functools
import math

import jax
import jax.numpy as jnp
import numpy as np
from jax import lax
from jax.experimental import pallas as pl
from jax.experimental.pallas import tpu as pltpu
from jax.sharding import PartitionSpec as P

HD = 128
MESH = pl.DeviceIdType.MESH
rope_base = 1000000.0
VMEM = pltpu.VMEM
LAG = 1


def rope_tables(rows, blocks):
    half = HD // 2
    inv = rope_base ** (-(np.arange(half, dtype=np.float64) * 2.0) / HD)
    inv = np.concatenate([inv, inv])[None, :]
    near = np.arange(rows)[:, None] * inv
    far = np.arange(blocks)[:, None] * rows * inv
    near = np.stack([np.cos(near), np.sin(near)]).astype(np.float32)
    far = np.stack([np.cos(far), np.sin(far)])[:, :, None, :].astype(np.float32)
    return near, far


def attend(
    seq_count, tp_count, reach, chunk,
    tokens_hbm, gain_ref, wq_hbm, qb_ref, wk_hbm, kb_ref, wv_hbm, vb_ref, wo_hbm,
    kdoc_ref, near_hbm, far_ref, out_ref,
    tokens, normed, wq, wkv, wo, near, q_ref, kv_ref, kv_in, sent, got, own,
    load_sems, kv_send, kv_pass, kv_recv, send_sem, recv_sem,
):
    place = lax.axis_index("seq")
    turn = lax.axis_index("tp")
    rows, width = q_ref.shape
    heads = width // HD
    cols = out_ref.shape[1]
    parts = rows // chunk
    step = 2 * HD
    spans = [(lo, min(step, width - lo)) for lo in range(0, width, step)]
    loads = [
        pltpu.make_async_copy(tokens_hbm, tokens, load_sems.at[0]),
        pltpu.make_async_copy(wk_hbm, wkv.at[:, pl.ds(0, HD)], load_sems.at[1]),
        pltpu.make_async_copy(wv_hbm, wkv.at[:, pl.ds(HD, HD)], load_sems.at[2]),
        pltpu.make_async_copy(near_hbm, near, load_sems.at[3]),
    ]
    for index, (lo, size) in enumerate(spans):
        cut = pl.ds(lo, size)
        loads.append(
            pltpu.make_async_copy(wq_hbm.at[:, cut], wq.at[:, cut], load_sems.at[4 + index])
        )
    load = pltpu.make_async_copy(wo_hbm, wo, load_sems.at[4 + len(spans)])
    loads.append(load)
    for copy in loads:
        copy.start()

    barrier = pltpu.get_barrier_semaphore()
    span = min(reach + 1, seq_count - 1)
    for away in range(1, span + 1):
        @pl.when(place >= away)
        def _():
            pl.semaphore_signal(barrier, inc=1, device_id={"seq": place - away}, device_id_type=MESH)

        @pl.when(place + away < seq_count)
        def _():
            pl.semaphore_signal(barrier, inc=1, device_id={"seq": place + away}, device_id_type=MESH)

    @pl.when(turn > 0)
    def _():
        pl.semaphore_signal(barrier, inc=1, device_id={"tp": turn - 1}, device_id_type=MESH)

    @pl.when(turn < tp_count - 1)
    def _():
        pl.semaphore_signal(barrier, inc=1, device_id={"tp": turn + 1}, device_id_type=MESH)

    behind = jnp.minimum(place, reach)
    near_count = jnp.minimum(place, span) + jnp.minimum(seq_count - 1 - place, span)
    sides = jnp.where(turn > 0, 1, 0) + jnp.where(turn < tp_count - 1, 1, 0)

    loads[0].wait()
    slab = 64
    gain = gain_ref[...].reshape(1, gain_ref.shape[0])

    @pl.loop(0, rows // slab)
    def _(index):
        cut = pl.ds(pl.multiple_of(index * slab, slab), slab)
        wide = tokens[cut, :].astype(jnp.float32)
        mean = jnp.mean(wide * wide, axis=-1, keepdims=True)
        normed[cut, :] = (wide * lax.rsqrt(mean + 1e-06) * gain).astype(jnp.bfloat16)

    loads[3].wait()
    far_cos, far_sin = far_ref[0, place], far_ref[1, place]
    cos = near[0] * far_cos - near[1] * far_sin
    sin = near[1] * far_cos + near[0] * far_sin
    lane = lax.broadcasted_iota(jnp.int32, (rows, HD), 1)
    near[0] = cos
    near[1] = jnp.where(lane < HD // 2, -sin, sin)

    def rope(t):
        return (t * near[0] + pltpu.roll(t, HD // 2, 1) * near[1]).astype(jnp.bfloat16)

    loads[1].wait()
    loads[2].wait()
    kv = jnp.dot(normed[...], wkv[...], preferred_element_type=jnp.float32)
    kv_ref[0] = rope(kv[:, :HD] + kb_ref[...].reshape(1, HD))
    kv_ref[1] = (kv[:, HD:] + vb_ref[...].reshape(1, HD)).astype(jnp.bfloat16)

    pl.semaphore_wait(barrier, near_count + sides)

    odd = lax.rem(place, 2) == 1
    partner = place + 1 - 2 * lax.rem(place, 2)

    def kv_copy(away):
        return pltpu.make_async_remote_copy(
            src_ref=kv_ref, dst_ref=kv_in.at[away - 1],
            send_sem=kv_send.at[away - 1], recv_sem=kv_recv.at[away - 1],
            device_id={"seq": lax.rem(place + away, seq_count)}, device_id_type=MESH,
        )

    def relay(away, landing):
        return pltpu.make_async_remote_copy(
            src_ref=kv_in.at[away - 1], dst_ref=kv_in.at[landing - 1],
            send_sem=kv_pass.at[away - 1], recv_sem=kv_recv.at[landing - 1],
            device_id={"seq": partner}, device_id_type=MESH,
        )

    evens = [away for away in range(2, reach + 2, 2) if away < seq_count]

    def wanted(away):
        return odd if away > reach else (place >= 0)

    def each_send(act):
        for away in evens:
            @pl.when((place + away < seq_count) & wanted(away))
            def _():
                act(kv_copy(away))

        @pl.when(jnp.logical_not(odd))
        def _():
            act(kv_copy(1))

    def each_relay(act):
        for away in evens:
            if away + 1 <= reach:
                @pl.when((place >= away) & jnp.logical_not(odd))
                def _():
                    act(relay(away, away + 1))

            @pl.when((place >= away) & odd)
            def _():
                act(relay(away, away - 1))

    each_send(lambda copy: copy.start())

    for index, (lo, size) in enumerate(spans):
        loads[4 + index].wait()
        out = jnp.dot(
            normed[...], wq[:, lo:lo + size], preferred_element_type=jnp.float32
        ) + qb_ref[lo:lo + size].reshape(1, size)
        for head in range(0, size, HD):
            q_ref[:, lo + head:lo + head + HD] = rope(out[:, head:head + HD])

    for away in evens:
        @pl.when((place >= away) & wanted(away))
        def _():
            kv_copy(away).wait_recv()

        if away + 1 <= reach:
            @pl.when((place >= away) & jnp.logical_not(odd))
            def _():
                relay(away, away + 1).start()

        @pl.when((place >= away) & odd)
        def _():
            relay(away, away - 1).start()

    def term_copy(side, dest, part):
        cut = pl.ds(pl.multiple_of(part * chunk, chunk), chunk)
        target = lax.rem(turn + (1 if side == 0 else tp_count - 1), tp_count)
        return pltpu.make_async_remote_copy(
            src_ref=sent.at[dest, cut], dst_ref=got.at[side, dest, cut],
            send_sem=send_sem.at[dest, part], recv_sem=recv_sem.at[side, dest, part],
            device_id={"tp": target}, device_id_type=MESH,
        )

    factor = math.log2(math.e) / HD**0.5
    order = sorted(range(tp_count), key=lambda d: (-abs(2 * d - tp_count + 1), -d))

    def forward(part):
        cut = pl.ds(pl.multiple_of(part * chunk, chunk), chunk)
        for dest in order:
            for side in (0, 1):
                inner = (turn > 0) & (dest > turn) if side == 0 else (
                    (turn < tp_count - 1) & (dest < turn))

                @pl.when(inner)
                def _():
                    term_copy(side, dest, part).wait_recv()
                    sent[dest, cut] = (
                        sent[dest, cut].astype(jnp.float32) + got[side, dest, cut].astype(jnp.float32)
                    ).astype(jnp.bfloat16)
                    term_copy(side, dest, part).start()

    def finish(part):
        cut = pl.ds(pl.multiple_of(part * chunk, chunk), chunk)
        for dest in range(tp_count):
            for side in (0, 1):
                edge = (turn > 0) if side == 0 else (turn < tp_count - 1)

                @pl.when((dest == turn) & edge)
                def _():
                    term_copy(side, dest, part).wait_recv()
                    own[cut, :] = own[cut, :] + got[side, dest, cut].astype(jnp.float32)

        out_ref[cut, :] = own[cut, :].astype(jnp.bfloat16)

    def piece(part):
        cut = pl.ds(pl.multiple_of(part * chunk, chunk), chunk)
        q = jnp.concatenate([q_ref[cut, h * HD:(h + 1) * HD] for h in range(heads)], axis=0)
        lanes = kdoc_ref[place, :, cut].astype(jnp.float32)
        qdoc = jnp.broadcast_to(lanes, (chunk, chunk)).T[:, :1]

        def block(state, k, v, visible):
            top, total, summed = state
            s = lax.dot_general(q, k, (((1,), (1,)), ((), ())), preferred_element_type=jnp.float32)
            s = s.reshape(heads, chunk, rows) * factor
            s = jnp.where(visible[None], s, -1e30)
            fresh = jnp.maximum(top, jnp.max(s, axis=-1, keepdims=True))
            e = jnp.exp2(s - fresh)
            scale = jnp.exp2(top - fresh)
            total = total * scale + jnp.sum(e, axis=-1, keepdims=True)
            pv = jnp.dot(
                e.astype(jnp.bfloat16).reshape(heads * chunk, rows), v,
                preferred_element_type=jnp.float32,
            )
            return fresh, total, summed * scale + pv.reshape(heads, chunk, HD)

        row = part * chunk + lax.broadcasted_iota(jnp.int32, (chunk, rows), 0)
        col = lax.broadcasted_iota(jnp.int32, (chunk, rows), 1)
        state = (
            jnp.full((heads, chunk, 1), -1e30, jnp.float32),
            jnp.zeros((heads, chunk, 1), jnp.float32),
            jnp.zeros((heads, chunk, HD), jnp.float32),
        )
        state = block(
            state, kv_ref[0], kv_ref[1], (col <= row) & (qdoc == kdoc_ref[place].astype(jnp.float32))
        )

        def earlier(away, state):
            @pl.when((part == 0) & (lax.rem(away, 2) == 1))
            def _():
                kv_copy(away).wait_recv()

            return block(
                state, kv_in[away - 1, 0], kv_in[away - 1, 1],
                qdoc == kdoc_ref[place - away].astype(jnp.float32),
            )

        _, total, summed = lax.fori_loop(1, behind + 1, earlier, state)
        context = (summed / total).astype(jnp.bfloat16)
        context = jnp.concatenate([context[h] for h in range(heads)], axis=1)

        @pl.when(part == 0)
        def _():
            load.wait()

        for dest in order:
            term = jnp.dot(
                context, wo[:, dest * cols:(dest + 1) * cols], preferred_element_type=jnp.float32
            )

            @pl.when(dest == turn)
            def _():
                own[cut, :] = term

            @pl.when(dest != turn)
            def _():
                sent[dest, cut] = term.astype(jnp.bfloat16)

            @pl.when((turn == 0) & (dest > 0))
            def _():
                term_copy(0, dest, part).start()

            @pl.when((turn == tp_count - 1) & (dest < tp_count - 1))
            def _():
                term_copy(1, dest, part).start()

    @pl.loop(0, parts + LAG)
    def _(part):
        @pl.when(part < parts)
        def _():
            piece(part)

        @pl.when(part >= LAG)
        def _():
            forward(part - LAG)

    @pl.loop(0, parts)
    def _(part):
        finish(part)

    @pl.loop(0, parts)
    def _(part):
        for dest in range(tp_count):
            @pl.when(dest != turn)
            def _():
                term_copy(0, dest, part).wait_send()

    each_send(lambda copy: copy.wait_send())
    each_relay(lambda copy: copy.wait_send())


def body(
    tokens, norm_gain, q_weight, q_bias, k_weight, k_bias, v_weight, v_bias, o_weight, doc_ids
):
    rows, model = tokens.shape
    seq_count = lax.axis_size("seq")
    tp_count = lax.axis_size("tp")
    width = q_weight.shape[1]
    cols = o_weight.shape[1] // tp_count
    reach = min(seq_count - 1, (seq_count * rows // 2 + 2 * rows - 2) // rows)
    chunk = rows // 4
    parts = rows // chunk
    near, far = rope_tables(rows, seq_count)
    hbm = pl.BlockSpec(memory_space=pl.ANY)
    vmem = pl.BlockSpec(memory_space=VMEM)
    slots = reach + 1
    spans = -(-width // (2 * HD))
    kdoc = doc_ids.reshape(seq_count, 1, rows)
    return pl.pallas_call(
        functools.partial(attend, seq_count, tp_count, reach, chunk),
        out_shape=jax.ShapeDtypeStruct((rows, cols), jnp.bfloat16),
        in_specs=[hbm, vmem, hbm, vmem, hbm, vmem, hbm, vmem, hbm, vmem, hbm, vmem],
        out_specs=vmem,
        scratch_shapes=[
            VMEM((rows, model), jnp.bfloat16),
            VMEM((rows, model), jnp.bfloat16),
            VMEM((model, width), jnp.bfloat16),
            VMEM((model, 2 * HD), jnp.bfloat16),
            VMEM(o_weight.shape, jnp.bfloat16),
            VMEM((2, rows, HD), jnp.float32),
            VMEM((rows, width), jnp.bfloat16),
            VMEM((2, rows, HD), jnp.bfloat16),
            VMEM((slots, 2, rows, HD), jnp.bfloat16),
            VMEM((tp_count, rows, cols), jnp.bfloat16),
            VMEM((2, tp_count, rows, cols), jnp.bfloat16),
            VMEM((rows, cols), jnp.float32),
            pltpu.SemaphoreType.DMA((5 + spans,)),
            pltpu.SemaphoreType.DMA((slots,)),
            pltpu.SemaphoreType.DMA((slots,)),
            pltpu.SemaphoreType.DMA((slots,)),
            pltpu.SemaphoreType.DMA((tp_count, parts)),
            pltpu.SemaphoreType.DMA((2, tp_count, parts)),
        ],
        compiler_params=pltpu.CompilerParams(
            collective_id=0, has_side_effects=True, vmem_limit_bytes=56 * 1024 * 1024
        ),
    )(
        tokens, norm_gain, q_weight, q_bias, k_weight, k_bias, v_weight, v_bias, o_weight,
        kdoc, jnp.asarray(near), jnp.asarray(far),
    )


def solution(mesh):
    placed = (
        P("seq", None),
        P(),
        P(None, "tp"),
        P("tp"),
        P(None, "tp"),
        P("tp"),
        P(None, "tp"),
        P("tp"),
        P("tp", None),
        P(),
    )
    return jax.shard_map(
        body, mesh=mesh, in_specs=placed, out_specs=P("seq", "tp"), check_vma=False
    )
```

```python
import functools
import math

import jax
import jax.numpy as jnp
import numpy as np
from jax import lax
from jax.experimental import pallas as pl
from jax.experimental.pallas import tpu as pltpu
from jax.sharding import PartitionSpec as P

HD = 128
MESH = pl.DeviceIdType.MESH
rope_base = 1000000.0
VMEM = pltpu.VMEM
LAG = 1


def rope_tables(rows, blocks):
    half = HD // 2
    inv = rope_base ** (-(np.arange(half, dtype=np.float64) * 2.0) / HD)
    inv = np.concatenate([inv, inv])[None, :]
    near = np.arange(rows)[:, None] * inv
    far = np.arange(blocks)[:, None] * rows * inv
    near = np.stack([np.cos(near), np.sin(near)]).astype(np.float32)
    far = np.stack([np.cos(far), np.sin(far)])[:, :, None, :].astype(np.float32)
    return near, far


def attend(
    seq_count, tp_count, reach, chunk,
    tokens_hbm, gain_ref, wq_hbm, qb_ref, wk_hbm, kb_ref, wv_hbm, vb_ref, wo_hbm,
    kdoc_ref, near_hbm, far_ref, out_ref,
    tokens, normed, wq, wkv, wo, near, q_ref, kv_ref, kv_in, sent, got, own,
    load_sems, kv_send, kv_pass, kv_recv, send_sem, recv_sem,
):
    place = lax.axis_index("seq")
    turn = lax.axis_index("tp")
    rows, width = q_ref.shape
    heads = width // HD
    cols = out_ref.shape[1]
    parts = rows // chunk
    step = 2 * HD
    spans = [(lo, min(step, width - lo)) for lo in range(0, width, step)]
    loads = [
        pltpu.make_async_copy(tokens_hbm, tokens, load_sems.at[0]),
        pltpu.make_async_copy(wk_hbm, wkv.at[:, pl.ds(0, HD)], load_sems.at[1]),
        pltpu.make_async_copy(wv_hbm, wkv.at[:, pl.ds(HD, HD)], load_sems.at[2]),
        pltpu.make_async_copy(near_hbm, near, load_sems.at[3]),
    ]
    for index, (lo, size) in enumerate(spans):
        cut = pl.ds(lo, size)
        loads.append(
            pltpu.make_async_copy(wq_hbm.at[:, cut], wq.at[:, cut], load_sems.at[4 + index])
        )
    load = pltpu.make_async_copy(wo_hbm, wo, load_sems.at[4 + len(spans)])
    loads.append(load)
    for copy in loads:
        copy.start()

    barrier = pltpu.get_barrier_semaphore()
    span = min(reach + 1, seq_count - 1)
    for away in range(1, span + 1):
        @pl.when(place >= away)
        def _():
            pl.semaphore_signal(barrier, inc=1, device_id={"seq": place - away}, device_id_type=MESH)

        @pl.when(place + away < seq_count)
        def _():
            pl.semaphore_signal(barrier, inc=1, device_id={"seq": place + away}, device_id_type=MESH)

    @pl.when(turn > 0)
    def _():
        pl.semaphore_signal(barrier, inc=1, device_id={"tp": turn - 1}, device_id_type=MESH)

    @pl.when(turn < tp_count - 1)
    def _():
        pl.semaphore_signal(barrier, inc=1, device_id={"tp": turn + 1}, device_id_type=MESH)

    behind = jnp.minimum(place, reach)
    near_count = jnp.minimum(place, span) + jnp.minimum(seq_count - 1 - place, span)
    sides = jnp.where(turn > 0, 1, 0) + jnp.where(turn < tp_count - 1, 1, 0)

    loads[0].wait()
    slab = 64
    gain = gain_ref[...].reshape(1, gain_ref.shape[0])

    @pl.loop(0, rows // slab)
    def _(index):
        cut = pl.ds(pl.multiple_of(index * slab, slab), slab)
        wide = tokens[cut, :].astype(jnp.float32)
        mean = jnp.mean(wide * wide, axis=-1, keepdims=True)
        normed[cut, :] = (wide * lax.rsqrt(mean + 1e-06) * gain).astype(jnp.bfloat16)

    loads[3].wait()
    far_cos, far_sin = far_ref[0, place], far_ref[1, place]
    cos = near[0] * far_cos - near[1] * far_sin
    sin = near[1] * far_cos + near[0] * far_sin
    lane = lax.broadcasted_iota(jnp.int32, (rows, HD), 1)
    near[0] = cos
    near[1] = jnp.where(lane < HD // 2, -sin, sin)

    def rope(t):
        return (t * near[0] + pltpu.roll(t, HD // 2, 1) * near[1]).astype(jnp.bfloat16)

    loads[1].wait()
    loads[2].wait()
    kv = jnp.dot(normed[...], wkv[...], preferred_element_type=jnp.float32)
    kv_ref[0] = rope(kv[:, :HD] + kb_ref[...].reshape(1, HD))
    kv_ref[1] = (kv[:, HD:] + vb_ref[...].reshape(1, HD)).astype(jnp.bfloat16)

    pl.semaphore_wait(barrier, near_count + sides)

    odd = lax.rem(place, 2) == 1
    partner = place + 1 - 2 * lax.rem(place, 2)

    def kv_copy(away):
        return pltpu.make_async_remote_copy(
            src_ref=kv_ref, dst_ref=kv_in.at[away - 1],
            send_sem=kv_send.at[away - 1], recv_sem=kv_recv.at[away - 1],
            device_id={"seq": lax.rem(place + away, seq_count)}, device_id_type=MESH,
        )

    def relay(away, landing):
        return pltpu.make_async_remote_copy(
            src_ref=kv_in.at[away - 1], dst_ref=kv_in.at[landing - 1],
            send_sem=kv_pass.at[away - 1], recv_sem=kv_recv.at[landing - 1],
            device_id={"seq": partner}, device_id_type=MESH,
        )

    evens = [away for away in range(2, reach + 2, 2) if away < seq_count]

    def wanted(away):
        return odd if away > reach else (place >= 0)

    def each_send(act):
        for away in evens:
            @pl.when((place + away < seq_count) & wanted(away))
            def _():
                act(kv_copy(away))

        @pl.when(jnp.logical_not(odd))
        def _():
            act(kv_copy(1))

    def each_relay(act):
        for away in evens:
            if away + 1 <= reach:
                @pl.when((place >= away) & jnp.logical_not(odd))
                def _():
                    act(relay(away, away + 1))

            @pl.when((place >= away) & odd)
            def _():
                act(relay(away, away - 1))

    each_send(lambda copy: copy.start())

    for index, (lo, size) in enumerate(spans):
        loads[4 + index].wait()
        out = jnp.dot(
            normed[...], wq[:, lo:lo + size], preferred_element_type=jnp.float32
        ) + qb_ref[lo:lo + size].reshape(1, size)
        for head in range(0, size, HD):
            q_ref[:, lo + head:lo + head + HD] = rope(out[:, head:head + HD])

    for away in evens:
        @pl.when((place >= away) & wanted(away))
        def _():
            kv_copy(away).wait_recv()

        if away + 1 <= reach:
            @pl.when((place >= away) & jnp.logical_not(odd))
            def _():
                relay(away, away + 1).start()

        @pl.when((place >= away) & odd)
        def _():
            relay(away, away - 1).start()

    def term_copy(side, dest, part):
        cut = pl.ds(pl.multiple_of(part * chunk, chunk), chunk)
        target = lax.rem(turn + (1 if side == 0 else tp_count - 1), tp_count)
        return pltpu.make_async_remote_copy(
            src_ref=sent.at[dest, cut], dst_ref=got.at[side, dest, cut],
            send_sem=send_sem.at[dest, part], recv_sem=recv_sem.at[side, dest, part],
            device_id={"tp": target}, device_id_type=MESH,
        )

    factor = math.log2(math.e) / HD**0.5
    order = sorted(range(tp_count), key=lambda d: (-abs(2 * d - tp_count + 1), -d))

    def forward(part, first):
        cut = pl.ds(pl.multiple_of(part * chunk, chunk), chunk)
        for side in (0, 1):
            chosen = (2 * turn < tp_count) if (side == 0) == first else (2 * turn >= tp_count)
            for dest in order:
                inner = (turn > 0) & (dest > turn) if side == 0 else (
                    (turn < tp_count - 1) & (dest < turn))

                @pl.when(inner & chosen)
                def _():
                    term_copy(side, dest, part).wait_recv()
                    sent[dest, cut] = (
                        sent[dest, cut].astype(jnp.float32) + got[side, dest, cut].astype(jnp.float32)
                    ).astype(jnp.bfloat16)
                    term_copy(side, dest, part).start()

    def finish(part):
        cut = pl.ds(pl.multiple_of(part * chunk, chunk), chunk)
        for dest in range(tp_count):
            for side in (0, 1):
                edge = (turn > 0) if side == 0 else (turn < tp_count - 1)

                @pl.when((dest == turn) & edge)
                def _():
                    term_copy(side, dest, part).wait_recv()
                    own[cut, :] = own[cut, :] + got[side, dest, cut].astype(jnp.float32)

        out_ref[cut, :] = own[cut, :].astype(jnp.bfloat16)

    def piece(part):
        cut = pl.ds(pl.multiple_of(part * chunk, chunk), chunk)
        q = jnp.concatenate([q_ref[cut, h * HD:(h + 1) * HD] for h in range(heads)], axis=0)
        lanes = kdoc_ref[place, :, cut].astype(jnp.float32)
        qdoc = jnp.broadcast_to(lanes, (chunk, chunk)).T[:, :1]

        def block(state, k, v, visible):
            top, total, summed = state
            s = lax.dot_general(q, k, (((1,), (1,)), ((), ())), preferred_element_type=jnp.float32)
            s = s.reshape(heads, chunk, rows) * factor
            s = jnp.where(visible[None], s, -1e30)
            fresh = jnp.maximum(top, jnp.max(s, axis=-1, keepdims=True))
            e = jnp.exp2(s - fresh)
            scale = jnp.exp2(top - fresh)
            total = total * scale + jnp.sum(e, axis=-1, keepdims=True)
            pv = jnp.dot(
                e.astype(jnp.bfloat16).reshape(heads * chunk, rows), v,
                preferred_element_type=jnp.float32,
            )
            return fresh, total, summed * scale + pv.reshape(heads, chunk, HD)

        row = part * chunk + lax.broadcasted_iota(jnp.int32, (chunk, rows), 0)
        col = lax.broadcasted_iota(jnp.int32, (chunk, rows), 1)
        state = (
            jnp.full((heads, chunk, 1), -1e30, jnp.float32),
            jnp.zeros((heads, chunk, 1), jnp.float32),
            jnp.zeros((heads, chunk, HD), jnp.float32),
        )
        state = block(
            state, kv_ref[0], kv_ref[1], (col <= row) & (qdoc == kdoc_ref[place].astype(jnp.float32))
        )

        def earlier(away, state):
            @pl.when((part == 0) & (lax.rem(away, 2) == 1))
            def _():
                kv_copy(away).wait_recv()

            return block(
                state, kv_in[away - 1, 0], kv_in[away - 1, 1],
                qdoc == kdoc_ref[place - away].astype(jnp.float32),
            )

        _, total, summed = lax.fori_loop(1, behind + 1, earlier, state)
        context = (summed / total).astype(jnp.bfloat16)
        context = jnp.concatenate([context[h] for h in range(heads)], axis=1)

        @pl.when(part == 0)
        def _():
            load.wait()

        for dest in order:
            term = jnp.dot(
                context, wo[:, dest * cols:(dest + 1) * cols], preferred_element_type=jnp.float32
            )

            @pl.when(dest == turn)
            def _():
                own[cut, :] = term

            @pl.when(dest != turn)
            def _():
                sent[dest, cut] = term.astype(jnp.bfloat16)

            @pl.when((turn == 0) & (dest > 0))
            def _():
                term_copy(0, dest, part).start()

            @pl.when((turn == tp_count - 1) & (dest < tp_count - 1))
            def _():
                term_copy(1, dest, part).start()

    @pl.loop(0, parts + LAG + 1)
    def _(part):
        @pl.when(part < parts)
        def _():
            piece(part)

        @pl.when((part >= LAG) & (part < parts + LAG))
        def _():
            forward(part - LAG, True)

        @pl.when(part >= LAG + 1)
        def _():
            forward(part - LAG - 1, False)

    @pl.loop(0, parts)
    def _(part):
        finish(part)

    @pl.loop(0, parts)
    def _(part):
        for dest in range(tp_count):
            @pl.when(dest != turn)
            def _():
                term_copy(0, dest, part).wait_send()

    each_send(lambda copy: copy.wait_send())
    each_relay(lambda copy: copy.wait_send())


def body(
    tokens, norm_gain, q_weight, q_bias, k_weight, k_bias, v_weight, v_bias, o_weight, doc_ids
):
    rows, model = tokens.shape
    seq_count = lax.axis_size("seq")
    tp_count = lax.axis_size("tp")
    width = q_weight.shape[1]
    cols = o_weight.shape[1] // tp_count
    reach = min(seq_count - 1, (seq_count * rows // 2 + 2 * rows - 2) // rows)
    chunk = rows // 4
    parts = rows // chunk
    near, far = rope_tables(rows, seq_count)
    hbm = pl.BlockSpec(memory_space=pl.ANY)
    vmem = pl.BlockSpec(memory_space=VMEM)
    slots = reach + 1
    spans = -(-width // (2 * HD))
    kdoc = doc_ids.reshape(seq_count, 1, rows)
    return pl.pallas_call(
        functools.partial(attend, seq_count, tp_count, reach, chunk),
        out_shape=jax.ShapeDtypeStruct((rows, cols), jnp.bfloat16),
        in_specs=[hbm, vmem, hbm, vmem, hbm, vmem, hbm, vmem, hbm, vmem, hbm, vmem],
        out_specs=vmem,
        scratch_shapes=[
            VMEM((rows, model), jnp.bfloat16),
            VMEM((rows, model), jnp.bfloat16),
            VMEM((model, width), jnp.bfloat16),
            VMEM((model, 2 * HD), jnp.bfloat16),
            VMEM(o_weight.shape, jnp.bfloat16),
            VMEM((2, rows, HD), jnp.float32),
            VMEM((rows, width), jnp.bfloat16),
            VMEM((2, rows, HD), jnp.bfloat16),
            VMEM((slots, 2, rows, HD), jnp.bfloat16),
            VMEM((tp_count, rows, cols), jnp.bfloat16),
            VMEM((2, tp_count, rows, cols), jnp.bfloat16),
            VMEM((rows, cols), jnp.float32),
            pltpu.SemaphoreType.DMA((5 + spans,)),
            pltpu.SemaphoreType.DMA((slots,)),
            pltpu.SemaphoreType.DMA((slots,)),
            pltpu.SemaphoreType.DMA((slots,)),
            pltpu.SemaphoreType.DMA((tp_count, parts)),
            pltpu.SemaphoreType.DMA((2, tp_count, parts)),
        ],
        compiler_params=pltpu.CompilerParams(
            collective_id=0, has_side_effects=True, vmem_limit_bytes=56 * 1024 * 1024
        ),
    )(
        tokens, norm_gain, q_weight, q_bias, k_weight, k_bias, v_weight, v_bias, o_weight,
        kdoc, jnp.asarray(near), jnp.asarray(far),
    )


def solution(mesh):
    placed = (
        P("seq", None),
        P(),
        P(None, "tp"),
        P("tp"),
        P(None, "tp"),
        P("tp"),
        P(None, "tp"),
        P("tp"),
        P("tp", None),
        P(),
    )
    return jax.shard_map(
        body, mesh=mesh, in_specs=placed, out_specs=P("seq", "tp"), check_vma=False
    )
```
